32 devices in a mesh: dp: 4 (over y, core), vocab: 8 (over z, x).
Axes of the slice: x: 2, y: 2, z: 4, core: 2. Of those that a mesh axis runs over, the one named last changes fastest.
Arguments:
- hidden: bfloat16 [256, 3584], P('dp'), may hold values from -48 to 48
- embedding: bfloat16 [24576, 3584], P(('dp', 'vocab')), may hold values from -1 to 1
- targets: int32 [256], P('dp'), may hold values from 0 to 24575
- loss_weight: bfloat16 [256], P('dp'), may hold values from 1 to 10
Outputs:
- hidden_grad: bfloat16 [256, 3584], P('dp')
- table_grad: bfloat16 [24576, 3584], P(('dp', 'vocab'))
The draws below stay inside these ranges and needn't reach their ends.
All inputs are finite; a program needn't handle non-finite values.
Results may differ from the reference program's by a relative error of at most 0.0049.
Values may be sent and summed in bfloat16 or wider, within the bound.
A program may use at most 128 MiB of HBM per device.

```python
import math
import jax
import jax.numpy as jnp
import numpy as np
from jax import lax

D = 3584
VROWS = 768
VOCAB = 24576
TOKENS = 256
N_VOCAB = 8


def draw_hidden(key, part):
    noise = jnp.clip(jax.random.normal(jax.random.fold_in(key, 11), (TOKENS, D), jnp.float32), -6.0, 6.0)
    return noise.astype(jnp.bfloat16)


def draw_embedding(key, part):
    noise = jnp.clip(jax.random.normal(jax.random.fold_in(key, 13), (VOCAB, D), jnp.float32), -6.0, 6.0)
    place = jnp.arange(VOCAB, dtype=jnp.float32) / (VOCAB - 1)
    rising = jnp.sqrt(1.0 + 0.245 * place)
    table = noise * (3.0 / math.sqrt(D))
    return jnp.clip(table * rising[:, None], -1.0, 1.0).astype(jnp.bfloat16)


def with_ends(drawn, stream_key, low, top_value):
    extent = drawn.shape
    spot = [jax.random.randint(jax.random.fold_in(stream_key, axis), (), 0, extent[axis]) for axis in range(len(extent))]
    drawn = drawn.at[tuple(spot)].set(low)
    longest = extent.index(max(extent))
    spot[longest] = (spot[longest] + 1) % extent[longest]
    return drawn.at[tuple(spot)].set(top_value)


def levels(own_key, dims, pieces, low, top_value):
    gain, own = 1.0, jax.random.fold_in(own_key, 6)
    for position, parts in pieces:
        draws = jnp.exp(jax.random.uniform(jax.random.fold_in(own, position), (parts,), jnp.float32, low / len(pieces), top_value / len(pieces)))
        gain = gain * jnp.repeat(draws, dims[position] // parts).reshape([-1 if axis == position else 1 for axis in range(len(dims))])
    return gain


def cumulative_ranks(amount, slope):
    weights = [(1 << 20) // math.isqrt(standing ** slope) + 1 for standing in range(1, amount + 1)]
    scale = 1 + sum(weights) // (1 << 30)
    return np.cumsum(np.array([max(1, weight // scale) for weight in weights]))


def ranked_ids(rng, extent, number_of, skew):
    table = cumulative_ranks(number_of, skew)
    pick = jax.random.randint(jax.random.fold_in(rng, 1), extent, 0, int(table[number_of - 1]))
    grade = jnp.searchsorted(jnp.asarray(table, jnp.int32), pick, side="right")
    return jax.random.permutation(jax.random.fold_in(rng, 2), number_of)[grade].astype(jnp.int32)


def setup_inputs(seed: int = 0) -> dict:
    keys = jax.random.split(jax.random.key(seed), 5)
    hidden = draw_hidden(jax.random.fold_in(keys[4], 71), 0)
    embedding = draw_embedding(jax.random.fold_in(keys[4], 71), 0)
    targets = with_ends(ranked_ids(keys[2], (TOKENS,), VOCAB, 2), jax.random.fold_in(keys[2], 3), 0, VOCAB - 1).astype(jnp.int32)
    loss_weight = jnp.clip(jnp.exp(math.log(10.0) - 2.3025851 * jax.random.uniform(keys[3], (TOKENS,), jnp.float32) ** levels(keys[3], (TOKENS,), ((0, 4),), -0.2, 0.2)), 1.0, 10.0).astype(jnp.bfloat16)
    return dict(hidden=hidden, embedding=embedding, targets=targets, loss_weight=loss_weight)


soft_cap = 30.0
z_weight = 0.002


def capped_block(hidden, table_rows):
    logits = lax.dot_general(hidden, table_rows, (((1,), (1,)), ((), ())), preferred_element_type=jnp.float32)
    return soft_cap * jnp.tanh(logits / soft_cap)


def reference(hidden, embedding, targets, loss_weight):
    block_rows = VROWS * N_VOCAB
    table_blocks = embedding.reshape(VOCAB // block_rows, block_rows, D)

    def add_exp(exp_total, table_rows):
        capped = capped_block(hidden, table_rows)
        return exp_total + jnp.sum(jnp.exp(capped - soft_cap), axis=1), None

    exp_total, _ = lax.scan(add_exp, jnp.zeros((hidden.shape[0],), jnp.float32), table_blocks)
    weight = loss_weight.astype(jnp.float32)
    log_total = soft_cap + jnp.log(exp_total)
    factor = weight * (1.0 + 2.0 * z_weight * log_total) / exp_total

    def grads(accum_grad, blocks_item):
        table_rows, first_row = blocks_item
        capped = capped_block(hidden, table_rows)
        columns = first_row + jnp.arange(block_rows, dtype=jnp.int32)
        target_hit = targets[:, None] == columns[None, :]
        softmax_part = factor[:, None] * jnp.exp(capped - soft_cap) - jnp.where(target_hit, weight[:, None], 0.0)
        scores_grad = (softmax_part * (1.0 - (capped / soft_cap) ** 2)).astype(jnp.bfloat16)
        accum_grad = accum_grad + jnp.dot(scores_grad, table_rows, preferred_element_type=jnp.float32)
        rows_grad = lax.dot_general(scores_grad, hidden, (((0,), (0,)), ((), ())), preferred_element_type=jnp.float32)
        return accum_grad, rows_grad.astype(jnp.bfloat16)

    first_rows = jnp.arange(VOCAB // block_rows, dtype=jnp.int32) * block_rows
    hidden_sum, block_grads = lax.scan(grads, jnp.zeros(hidden.shape, jnp.float32), (table_blocks, first_rows))
    return hidden_sum.astype(jnp.bfloat16), block_grads.reshape(VOCAB, D)
```

```python
import functools

import jax
import jax.numpy as jnp
from jax import lax
from jax.experimental import pallas as pl
from jax.experimental.pallas import tpu as pltpu
from jax.sharding import PartitionSpec as P

soft_cap = 30.0
z_weight = 0.002
MESH = pl.DeviceIdType.MESH
f32, bf16 = jnp.float32, jnp.bfloat16


def kernel(cfg, hidden, embedding, marks, hgrad, tgrad,
           hid, emb, tw, pd, pv, uT, eT, sT, sN, gF, sC, rC, sY, rY, bF, sX, rX, sZ, rZ, out, tg,
           loc, tw_s, tw_r, hc_s, hc_r, hy_s, hy_r, hf_s, hf_r, pd_s, pd_r, pv_s, pv_r,
           c_s, c_r, y_s, y_r, x_s, x_r, z_s, z_r, az_s, az_r, ax_s, ax_r, tg_s):
    nd, nv, full, ck, AQ, VB = cfg
    Y, Z = nd // 2, nv // 2
    rows, D = hidden.shape
    V = embedding.shape[0]
    K = D // ck
    G8 = rows // 8
    d, v = lax.axis_index("dp"), lax.axis_index("vocab")
    c, y = lax.rem(d, 2), d // 2
    x, z = lax.rem(v, 2), v // 2
    dev = lambda dd, vv: dict(device_id=(dd, vv), device_id_type=MESH)
    core = dev(y * 2 + 1 - c, v)
    xdev = dev(d, z * 2 + 1 - x)
    ydev = lambda k: dev(lax.rem(y + k, Y) * 2 + c, v)
    zdev = lambda k: dev(d, lax.rem(z + k, Z) * 2 + x)
    rdma = lambda s, t, ss, rs, dv: pltpu.make_async_remote_copy(src_ref=s, dst_ref=t, send_sem=ss, recv_sem=rs, **dv)

    own = pl.ds(pl.multiple_of(d * rows, rows), rows)
    load_h = pltpu.make_async_copy(hidden, hid.at[own], loc.at[0])
    load_h.start()
    load_e = pltpu.make_async_copy(embedding, emb, loc.at[1])
    load_e.start()
    barrier = pltpu.get_barrier_semaphore()
    for k in range(1, nd):
        pl.semaphore_signal(barrier, inc=1, **dev(lax.rem(d + k, nd), v))
    for k in range(1, nv):
        pl.semaphore_signal(barrier, inc=1, **dev(d, lax.rem(v + k, nv)))
    tw[0] = marks[...]
    load_h.wait()
    pl.semaphore_wait(barrier, nd + nv - 2)

    sends = []

    def go(copy):
        copy.start()
        sends.append(copy)
        return copy

    aq = rows // AQ
    part = lambda dd, q: pl.ds(pl.multiple_of(dd * rows + q * aq, aq), aq)
    hy = lambda k, q: rdma(hid.at[part(d, q)], hid.at[part(d, q)], hy_s.at[k - 1, q], hy_r.at[k - 1, q], ydev(k))
    for q in range(AQ):
        for k in range(1, Y):
            go(hy(k, q))
    hc = go(rdma(hid.at[own], hid.at[own], hc_s.at[0], hc_r.at[0], core))
    tws = [go(rdma(tw.at[0], tw.at[k], tw_s.at[k - 1], tw_r.at[k - 1], dev(lax.rem(d + k, nd), v))) for k in range(1, nd)]
    forwards = []
    for q in range(AQ):
        for k in range(1, Y):
            hy(k, q).wait_recv()
            src = lax.rem(y + Y - k, Y) * 2 + c
            forwards.append(go(rdma(hid.at[part(src, q)], hid.at[part(src, q)], hf_s.at[k - 1, q], hf_r.at[k - 1, q], core)))
    hc.wait_recv()
    for copy in tws:
        copy.wait_recv()
    for copy in forwards:
        copy.wait_recv()
    load_e.wait()

    T = hid.shape[0]
    pd[0] = jnp.zeros_like(pd[0])

    def logits_block(b, carry):
        vb = pl.ds(pl.multiple_of(b * VB, VB), VB)
        lg = lax.dot_general(emb[vb, :], hid[...], (((1,), (1,)), ((), ())), preferred_element_type=f32)
        u = jnp.tanh(lg * (1.0 / soft_cap))
        e = jnp.exp(soft_cap * u - soft_cap)
        uT[vb, :] = 1.0 - u * u
        eT[vb, :] = e
        pd[0] += jnp.sum(e.reshape(VB // 8, 8, T), axis=0)
        return carry

    lax.fori_loop(0, V // VB, logits_block, 0)

    pds = [go(rdma(pd.at[0], pd.at[k], pd_s.at[k - 1], pd_r.at[k - 1], dev(lax.rem(d + k, nd), v))) for k in range(1, nd)]
    for copy in pds:
        copy.wait_recv()
    pv[0] = jnp.sum(pd[...], axis=0)
    pvs = [go(rdma(pv.at[0], pv.at[k], pv_s.at[k - 1], pv_r.at[k - 1], dev(d, lax.rem(v + k, nv)))) for k in range(1, nv)]
    for copy in pvs:
        copy.wait_recv()
    total = jnp.sum(jnp.sum(pv[...], axis=0), axis=0, keepdims=True)
    group = jnp.sum(tw[...], axis=0)
    weight, target = group[0:1, :], group[1:2, :]
    factor = weight * (1.0 + 2.0 * z_weight * (soft_cap + jnp.log(total))) / total
    first = (d * nv + v) * V

    def scores_block(b, carry):
        vb = pl.ds(pl.multiple_of(b * VB, VB), VB)
        cols = (first + b * VB + lax.broadcasted_iota(jnp.int32, (VB, T), 0)).astype(f32)
        s = (factor * eT[vb, :] - jnp.where(cols == target, weight, 0.0)) * uT[vb, :]
        sT[vb, :] = s.astype(bf16)
        sN[:, vb] = s.T.astype(bf16)
        return carry

    lax.fori_loop(0, V // VB, scores_block, 0)

    ccopy = lambda j: rdma(sC.at[j], rC.at[j], c_s.at[j], c_r.at[j], core)

    def grad_block(j, carry):
        g = jnp.dot(sN[...], emb[:, pl.ds(pl.multiple_of(j * ck, ck), ck)], preferred_element_type=f32)
        gF[j] = g.reshape(nd, rows, ck)
        for yy in range(Y):
            sC[j, yy] = gF[j, yy * 2 + 1 - c].astype(bf16)
        ccopy(j).start()
        return carry

    lax.fori_loop(0, K, grad_block, 0)
    ycopy = lambda j, k: rdma(sY.at[j, k - 1], rY.at[j, k - 1], y_s.at[j, k - 1], y_r.at[j, k - 1], ydev(k))

    def core_block(j, carry):
        ccopy(j).wait()
        for k in range(1, Y):
            yy = lax.rem(y + k, Y)
            sY[j, k - 1] = (gF[j, yy * 2 + c] + rC[j, yy].astype(f32)).astype(bf16)
            ycopy(j, k).start()
        return carry

    lax.fori_loop(0, K, core_block, 0)

    VT = V // VB
    tcopy = lambda b: pltpu.make_async_copy(tg.at[b], tgrad.at[pl.ds(pl.multiple_of(b * VB, VB), VB)], tg_s.at[b])

    def table_block(b, carry):
        vb = pl.ds(pl.multiple_of(b * VB, VB), VB)
        for j in range(K):
            cs = pl.ds(j * ck, ck)
            tg[b, :, cs] = jnp.dot(sT[vb, :], hid[:, cs], preferred_element_type=f32).astype(bf16)
        tcopy(b).start()
        return carry

    lax.fori_loop(0, VT, table_block, 0)

    def y_block(j):
        acc = gF[j, y * 2 + c] + rC[j, y].astype(f32)
        for k in range(1, Y):
            ycopy(j, k).wait()
            acc = acc + rY[j, k - 1].astype(f32)
        return acc

    if not full:
        for j in range(K):
            hgrad[:, j * ck:(j + 1) * ck] = y_block(j)
    else:
        h = G8 // 2
        gz = h // Z
        xcopy = lambda j: rdma(sX.at[j], rX.at[j], x_s.at[j], x_r.at[j], xdev)
        zcopy = lambda j, k: rdma(sZ.at[j, k - 1], rZ.at[j, k - 1], z_s.at[j, k - 1], z_r.at[j, k - 1], zdev(k))
        mine = lambda j: out.at[pl.ds(x * h + z * gz, gz), :, pl.ds(j * ck, ck)]
        half = lambda j: out.at[pl.ds(x * h, h), :, pl.ds(j * ck, ck)]
        azcopy = lambda j, k: rdma(mine(j), mine(j), az_s.at[j, k - 1], az_r.at[j, k - 1], zdev(k))
        axcopy = lambda j: rdma(half(j), half(j), ax_s.at[j], ax_r.at[j], xdev)
        xsum = lambda j, zz: bF[j, pl.ds(x * h + zz * gz, gz)] + rX[j, pl.ds(zz * gz, gz)].astype(f32)

        def stage0(j):
            bF[j] = y_block(j).reshape(G8, 8, ck)
            sX[j] = bF[j, pl.ds((1 - x) * h, h)].astype(bf16)
            xcopy(j).start()

        def stage1(j):
            xcopy(j).wait()
            for k in range(1, Z):
                sZ[j, k - 1] = xsum(j, lax.rem(z + k, Z)).astype(bf16)
                zcopy(j, k).start()

        def stage2(j):
            acc = xsum(j, z)
            for k in range(1, Z):
                zcopy(j, k).wait()
                acc = acc + rZ[j, k - 1].astype(f32)
            out[pl.ds(x * h + z * gz, gz), :, pl.ds(j * ck, ck)] = acc.astype(bf16)
            for k in range(1, Z):
                azcopy(j, k).start()

        def stage3(j):
            for k in range(1, Z):
                azcopy(j, k).wait()
            axcopy(j).start()

        def stage4(j):
            axcopy(j).wait()

        stages = [stage0, stage1, stage2, stage3, stage4]
        for s in range(K + len(stages) - 1):
            for i, stage in enumerate(stages):
                if 0 <= s - i < K:
                    stage(s - i)
        hgrad[...] = out[...]
    for b in range(VT):
        tcopy(b).wait()
    for copy in sends:
        copy.wait_send()


def body(hidden, embedding, targets, loss_weight):
    nd, nv = lax.axis_size("dp"), lax.axis_size("vocab")
    rows, D = hidden.shape
    V = embedding.shape[0]
    T = rows * nd
    Y, Z = nd // 2, nv // 2
    ck = next(s for s in (512, 256, 128, D) if D % s == 0)
    K = D // ck
    AQ = 2
    VB = next(s for s in (256, 128, V) if V % s == 0)
    G8 = rows // 8
    full = G8 % nv == 0
    d = lax.axis_index("dp")
    here = (lax.iota(jnp.int32, T) // rows == d)[None, :]
    line = jnp.stack([loss_weight.astype(f32), targets.astype(f32)])
    marks = jnp.pad(jnp.where(here, jnp.tile(line, (1, nd)), 0.0), ((0, 6), (0, 0)))
    h = G8 // 2
    gz = max(h // Z, 1)
    Zs, Ys = max(Z - 1, 1), max(Y - 1, 1)
    VM = pltpu.VMEM
    dma = lambda *shape: pltpu.SemaphoreType.DMA(shape)
    scratch = [
        VM((T, D), bf16), VM((V, D), bf16), VM((nd, 8, T), f32), VM((nd, 8, T), f32), VM((nv, 8, T), f32),
        VM((V, T), f32), VM((V, T), f32), VM((V, T), bf16), VM((T, V), bf16),
        VM((K, nd, rows, ck), f32), VM((K, Y, rows, ck), bf16), VM((K, Y, rows, ck), bf16),
        VM((K, Ys, rows, ck), bf16), VM((K, Ys, rows, ck), bf16),
        VM((K, G8, 8, ck), f32), VM((K, h, 8, ck), bf16), VM((K, h, 8, ck), bf16),
        VM((K, Zs, gz, 8, ck), bf16), VM((K, Zs, gz, 8, ck), bf16),
        VM((G8, 8, D), bf16), VM((V // VB, VB, D), bf16),
        dma(2), dma(nd), dma(nd), dma(1), dma(1), dma(Ys, AQ), dma(Ys, AQ), dma(Ys, AQ), dma(Ys, AQ),
        dma(nd), dma(nd), dma(nv), dma(nv),
        dma(K), dma(K), dma(K, Ys), dma(K, Ys), dma(K), dma(K), dma(K, Zs), dma(K, Zs), dma(K, Zs), dma(K, Zs), dma(K), dma(K),
        dma(V // VB),
    ]
    hshape = jax.ShapeDtypeStruct((G8, 8, D), bf16) if full else jax.ShapeDtypeStruct((rows, D), f32)
    any_spec = pl.BlockSpec(memory_space=pl.ANY)
    vmem_spec = pl.BlockSpec(memory_space=pltpu.VMEM)
    hgrad, tgrad = pl.pallas_call(
        functools.partial(kernel, (nd, nv, full, ck, AQ, VB)),
        out_shape=(hshape, jax.ShapeDtypeStruct((V, D), bf16)),
        in_specs=[any_spec, any_spec, vmem_spec],
        out_specs=(vmem_spec, any_spec),
        scratch_shapes=scratch,
        compiler_params=pltpu.CompilerParams(collective_id=0, has_side_effects=True, vmem_limit_bytes=60 * 1024 * 1024),
    )(hidden, embedding, marks)
    if full:
        return hgrad.reshape(rows, D), tgrad
    return lax.psum(hgrad, "vocab").astype(bf16), tgrad


def solution(mesh):
    return jax.shard_map(
        body,
        mesh=mesh,
        in_specs=(P("dp", None), P(("dp", "vocab"), None), P("dp"), P("dp")),
        out_specs=(P("dp", None), P(("dp", "vocab"), None)),
        check_vma=False,
    )
```

```python
import functools

import jax
import jax.numpy as jnp
from jax import lax
from jax.experimental import pallas as pl
from jax.experimental.pallas import tpu as pltpu
from jax.sharding import PartitionSpec as P

soft_cap = 30.0
z_weight = 0.002
MESH = pl.DeviceIdType.MESH
VMEM_LIMIT = 45
f32, bf16 = jnp.float32, jnp.bfloat16


def kernel(cfg, hidden, embedding, targets, weights, hgrad, tgrad,
           hid, emb, tw, pd, pv, uT, eT, sT, sN, gF, sC, rC, sY, rY, bF, sX, rX, sZ, rZ, out,
           loc, tw_s, tw_r, hc_s, hc_r, hy_s, hy_r, hf_s, hf_r, pd_s, pd_r, pv_s, pv_r,
           c_s, c_r, y_s, y_r, x_s, x_r, z_s, z_r, az_s, az_r, ax_s, ax_r):
    nd, nv, full, ck, NH, VB, TC = cfg
    Y, Z = nd // 2, nv // 2
    rows, D = hidden.shape
    V = embedding.shape[0]
    K = D // ck
    part = rows // NH
    TH = nd * part
    d, v = lax.axis_index("dp"), lax.axis_index("vocab")
    c, y = lax.rem(d, 2), d // 2
    x, z = lax.rem(v, 2), v // 2
    dev = lambda dd, vv: dict(device_id=(dd, vv), device_id_type=MESH)
    core = dev(y * 2 + 1 - c, v)
    xdev = dev(d, z * 2 + 1 - x)
    ydev = lambda k: dev(lax.rem(y + k, Y) * 2 + c, v)
    zdev = lambda k: dev(d, lax.rem(z + k, Z) * 2 + x)
    ddev = lambda k: dev(lax.rem(d + k, nd), v)
    vdev = lambda k: dev(d, lax.rem(v + k, nv))
    rdma = lambda s, t, ss, rs, dv: pltpu.make_async_remote_copy(src_ref=s, dst_ref=t, send_sem=ss, recv_sem=rs, **dv)

    block = lambda dd, a: hid.at[pl.ds(pl.multiple_of(a * TH + dd * part, part), part)]
    loads = [pltpu.make_async_copy(hidden.at[pl.ds(a * part, part)], block(d, a), loc.at[a]) for a in range(NH)]
    load_e = pltpu.make_async_copy(embedding, emb, loc.at[NH])
    for copy in loads:
        copy.start()
    load_e.start()
    barrier = pltpu.get_barrier_semaphore()
    for k in range(1, nd):
        pl.semaphore_signal(barrier, inc=1, **ddev(k))
    for k in range(1, nv):
        pl.semaphore_signal(barrier, inc=1, **vdev(k))
    T = NH * TH
    at = lax.broadcasted_iota(jnp.int32, (rows, T), 1)
    own = lax.broadcasted_iota(jnp.int32, (rows, T), 0)
    place = jnp.where((own // part) * TH + d * part + lax.rem(own, part) == at, 1.0, 0.0)
    line = jnp.concatenate([weights[...], targets[...].astype(f32), jnp.zeros((6, rows), f32)], axis=0)
    tw[0] = jnp.dot(line, place, precision=lax.Precision.HIGHEST, preferred_element_type=f32)
    for copy in loads:
        copy.wait()
    pl.semaphore_wait(barrier, nd + nv - 2)

    sends = []

    def go(copy):
        copy.start()
        sends.append(copy)
        return copy

    hy = lambda a, k: rdma(block(d, a), block(d, a), hy_s.at[a, k - 1], hy_r.at[a, k - 1], ydev(k))
    hc = lambda a: rdma(block(d, a), block(d, a), hc_s.at[a], hc_r.at[a], core)

    def hf(a, k):
        there = block(lax.rem(y + Y - k, Y) * 2 + c, a)
        return rdma(there, there, hf_s.at[a, k - 1], hf_r.at[a, k - 1], core)

    twc = lambda k: rdma(tw.at[0], tw.at[k], tw_s.at[k - 1], tw_r.at[k - 1], ddev(k))
    for k in range(1, nd):
        go(twc(k))
    for a in range(NH):
        for k in range(1, Y):
            go(hy(a, k))
        go(hc(a))

    def forward(a):
        for k in range(1, Y):
            hy(a, k).wait_recv()
            go(hf(a, k))

    def arrived(a):
        hc(a).wait_recv()
        for k in range(1, Y):
            hf(a, k).wait_recv()

    def logits(a):
        pd[a, 0] = jnp.zeros_like(pd[a, 0])

        def step(b, carry):
            vb = pl.ds(pl.multiple_of(b * VB, VB), VB)
            lg = lax.dot_general(emb[vb, :], hid[a * TH:(a + 1) * TH, :], (((1,), (1,)), ((), ())), preferred_element_type=f32)
            u = jnp.tanh(lg * (1.0 / soft_cap))
            e = jnp.exp(soft_cap * u - soft_cap)
            uT[a, vb, :] = 1.0 - u * u
            eT[a, vb, :] = e
            pd[a, 0] += jnp.sum(e.reshape(VB // 8, 8, TH), axis=0)
            return carry

        lax.fori_loop(0, V // VB, step, 0)

    pdc = lambda a, k: rdma(pd.at[a, 0], pd.at[a, k], pd_s.at[a, k - 1], pd_r.at[a, k - 1], ddev(k))
    pvc = lambda a, k: rdma(pv.at[a, 0], pv.at[a, k], pv_s.at[a, k - 1], pv_r.at[a, k - 1], vdev(k))

    def sums_out(a):
        for k in range(1, nd):
            go(pdc(a, k))

    def sums_on(a):
        for k in range(1, nd):
            pdc(a, k).wait_recv()
        pv[a, 0] = jnp.sum(pd[a], axis=0)
        for k in range(1, nv):
            go(pvc(a, k))

    first = (d * nv + v) * V

    def scores(a):
        for k in range(1, nv):
            pvc(a, k).wait_recv()
        total = jnp.sum(jnp.sum(pv[a], axis=0), axis=0, keepdims=True)
        group = jnp.sum(tw[:, :, a * TH:(a + 1) * TH], axis=0)
        weight, target = group[0:1, :], group[1:2, :]
        factor = weight * (1.0 + 2.0 * z_weight * (soft_cap + jnp.log(total))) / total

        def step(b, carry):
            vb = pl.ds(pl.multiple_of(b * VB, VB), VB)
            cols = (first + b * VB + lax.broadcasted_iota(jnp.int32, (VB, TH), 0)).astype(f32)
            s = (factor * eT[a, vb, :] - jnp.where(cols == target, weight, 0.0)) * uT[a, vb, :]
            sT[vb, a * TH:(a + 1) * TH] = s.astype(bf16)
            sN[a * TH:(a + 1) * TH, vb] = s.T.astype(bf16)
            return carry

        lax.fori_loop(0, V // VB, step, 0)

    ccopy = lambda i: rdma(sC.at[i], rC.at[i], c_s.at[i], c_r.at[i], core)
    ycopy = lambda i, k: rdma(sY.at[i, k - 1], rY.at[i, k - 1], y_s.at[i, k - 1], y_r.at[i, k - 1], ydev(k))

    def core_unit(i):
        ccopy(i).wait()
        for k in range(1, Y):
            yy = lax.rem(y + k, Y)
            sY[i, k - 1] = (gF[i, yy * 2 + c] + rC[i, yy].astype(f32)).astype(bf16)
            ycopy(i, k).start()

    def partials(a):
        def step(j, carry):
            i = a * K + j
            g = jnp.dot(sN[a * TH:(a + 1) * TH, :], emb[:, pl.ds(pl.multiple_of(j * ck, ck), ck)], preferred_element_type=f32)
            gF[i] = g.reshape(nd, part, ck)
            for yy in range(Y):
                sC[i, yy] = gF[i, yy * 2 + 1 - c].astype(bf16)
            ccopy(i).start()

            @pl.when(j >= 2)
            def _():
                core_unit(i - 2)

            return carry

        lax.fori_loop(0, K, step, 0)
        for j in range(max(K - 2, 0), K):
            core_unit(a * K + j)

    forward(0)
    for k in range(1, nd):
        twc(k).wait_recv()
    arrived(0)
    load_e.wait()
    logits(0)
    sums_out(0)
    for a in range(1, NH):
        forward(a)
        sums_on(a - 1)
        arrived(a)
        logits(a)
        sums_out(a)
        scores(a - 1)
        sums_on(a)
        partials(a - 1)
    if NH == 1:
        sums_on(0)
    scores(NH - 1)
    partials(NH - 1)

    pieces = [(b, j) for b in range(V // VB) for j in range(D // TC)]

    def table(b, j):
        vb, cs = pl.ds(b * VB, VB), pl.ds(j * TC, TC)
        tgrad[vb, cs] = jnp.dot(sT[vb, :], hid[:, cs], preferred_element_type=f32).astype(bf16)

    U = NH * K

    def y_unit(i):
        acc = gF[i, y * 2 + c] + rC[i, y].astype(f32)
        for k in range(1, Y):
            ycopy(i, k).wait()
            acc = acc + rY[i, k - 1].astype(f32)
        return acc

    if not full:
        for piece in pieces:
            table(*piece)
        for i in range(U):
            a, j = i // K, i % K
            hgrad[a * part:(a + 1) * part, j * ck:(j + 1) * ck] = y_unit(i)
    else:
        h = part // 8
        gz = h // Z
        cx = ck // 2
        xcopy = lambda i: rdma(sX.at[i], rX.at[i], x_s.at[i], x_r.at[i], xdev)
        zcopy = lambda i, k: rdma(sZ.at[i, k - 1], rZ.at[i, k - 1], z_s.at[i, k - 1], z_r.at[i, k - 1], zdev(k))
        mycols = lambda i: pl.ds(pl.multiple_of((i % K) * ck + x * cx, cx), cx)
        mine = lambda i: out.at[pl.ds((i // K) * h + z * gz, gz), :, mycols(i)]
        half = lambda i: out.at[pl.ds((i // K) * h, h), :, mycols(i)]
        azcopy = lambda i, k: rdma(mine(i), mine(i), az_s.at[i, k - 1], az_r.at[i, k - 1], zdev(k))
        axcopy = lambda i: rdma(half(i), half(i), ax_s.at[i], ax_r.at[i], xdev)
        xsum = lambda i, zz: bF[i, x, pl.ds(zz * gz, gz)] + rX[i, pl.ds(zz * gz, gz)].astype(f32)

        def stage0(i):
            acc = y_unit(i).reshape(h, 8, ck)
            for xx in range(2):
                bF[i, xx] = acc[:, :, xx * cx:(xx + 1) * cx]
            sX[i] = bF[i, 1 - x].astype(bf16)
            xcopy(i).start()

        def stage1(i):
            xcopy(i).wait()
            for k in range(1, Z):
                sZ[i, k - 1] = xsum(i, lax.rem(z + k, Z)).astype(bf16)
                zcopy(i, k).start()

        def stage2(i):
            acc = xsum(i, z)
            for k in range(1, Z):
                zcopy(i, k).wait()
                acc = acc + rZ[i, k - 1].astype(f32)
            out[pl.ds((i // K) * h + z * gz, gz), :, mycols(i)] = acc.astype(bf16)
            for k in range(1, Z):
                azcopy(i, k).start()

        def stage3(i):
            for k in range(1, Z):
                azcopy(i, k).wait()
            axcopy(i).start()

        plan = [(stage0, 0), (stage1, 3), (stage2, 8), (stage3, 13)]
        for s in range(U + plan[-1][1]):
            for _ in range(2):
                if pieces:
                    table(*pieces.pop())
            for stage, lag in plan:
                if 0 <= s - lag < U:
                    stage(s - lag)
        for piece in pieces:
            table(*piece)
        for i in range(U):
            axcopy(i).wait()
        hgrad[...] = out[...]
    for copy in sends:
        copy.wait_send()


def body(hidden, embedding, targets, loss_weight):
    nd, nv = lax.axis_size("dp"), lax.axis_size("vocab")
    rows, D = hidden.shape
    V = embedding.shape[0]
    T = rows * nd
    Y, Z = nd // 2, nv // 2
    ck = next(s for s in (512, 256, D) if D % s == 0)
    TC = next(s for s in (896, 512, 256, 128, D) if D % s == 0)
    K = D // ck
    NH = 2
    VB = next(s for s in (256, 128, V) if V % s == 0)
    part = rows // NH
    TH = nd * part
    U = NH * K
    full = (part // 8) % Z == 0
    h = part // 8
    gz = max(h // Z, 1)
    cx = ck // 2
    Zs, Ys = max(Z - 1, 1), max(Y - 1, 1)
    VM = pltpu.VMEM
    dma = lambda *shape: pltpu.SemaphoreType.DMA(shape)
    scratch = [
        VM((T, D), bf16), VM((V, D), bf16), VM((nd, 8, T), f32), VM((NH, nd, 8, TH), f32), VM((NH, nv, 8, TH), f32),
        VM((NH, V, TH), f32), VM((NH, V, TH), f32), VM((V, T), bf16), VM((T, V), bf16),
        VM((U, nd, part, ck), f32), VM((U, Y, part, ck), bf16), VM((U, Y, part, ck), bf16),
        VM((U, Ys, part, ck), bf16), VM((U, Ys, part, ck), bf16),
        VM((U, 2, h, 8, cx), f32), VM((U, h, 8, cx), bf16), VM((U, h, 8, cx), bf16),
        VM((U, Zs, gz, 8, cx), bf16), VM((U, Zs, gz, 8, cx), bf16),
        VM((NH * h, 8, D), bf16),
        dma(NH + 1), dma(nd), dma(nd), dma(NH), dma(NH), dma(NH, Ys), dma(NH, Ys), dma(NH, Ys), dma(NH, Ys),
        dma(NH, nd), dma(NH, nd), dma(NH, nv), dma(NH, nv),
        dma(U), dma(U), dma(U, Ys), dma(U, Ys), dma(U), dma(U), dma(U, Zs), dma(U, Zs), dma(U, Zs), dma(U, Zs), dma(U), dma(U),
    ]
    hshape = jax.ShapeDtypeStruct((NH * h, 8, D), bf16) if full else jax.ShapeDtypeStruct((rows, D), f32)
    any_spec = pl.BlockSpec(memory_space=pltpu.HBM)
    vmem_spec = pl.BlockSpec(memory_space=pltpu.VMEM)
    hgrad, tgrad = pl.pallas_call(
        functools.partial(kernel, (nd, nv, full, ck, NH, VB, TC)),
        out_shape=(hshape, jax.ShapeDtypeStruct((V, D), bf16)),
        in_specs=[any_spec, any_spec, vmem_spec, vmem_spec],
        out_specs=(vmem_spec, vmem_spec),
        scratch_shapes=scratch,
        compiler_params=pltpu.CompilerParams(collective_id=0, has_side_effects=True, vmem_limit_bytes=VMEM_LIMIT * 1024 * 1024),
    )(hidden, embedding, targets.reshape(1, rows), loss_weight.astype(f32).reshape(1, rows))
    if full:
        return hgrad.reshape(rows, D), tgrad
    return lax.psum(hgrad, "vocab").astype(bf16), tgrad


def solution(mesh):
    return jax.shard_map(
        body,
        mesh=mesh,
        in_specs=(P("dp", None), P(("dp", "vocab"), None), P("dp"), P("dp")),
        out_specs=(P("dp", None), P(("dp", "vocab"), None)),
        check_vma=False,
    )
```

```python
import functools

import jax
import jax.numpy as jnp
from jax import lax
from jax.experimental import pallas as pl
from jax.experimental.pallas import tpu as pltpu
from jax.sharding import PartitionSpec as P

soft_cap = 30.0
z_weight = 0.002
MESH = pl.DeviceIdType.MESH
VMEM_LIMIT = 45
f32, bf16 = jnp.float32, jnp.bfloat16


def kernel(cfg, hidden, embedding, targets, weights, hgrad, tgrad,
           hid, emb, tw, pd, pv, uT, eT, sT, sN, gF, sC, rC, sY, rY, bF, sX, rX, sZ, rZ, out,
           loc, tw_s, tw_r, hc_s, hc_r, hy_s, hy_r, hf_s, hf_r, pd_s, pd_r, pv_s, pv_r,
           c_s, c_r, y_s, y_r, x_s, x_r, z_s, z_r, az_s, az_r, ax_s, ax_r):
    nd, nv, full, ck, NH, VB, TC = cfg
    Y, Z = nd // 2, nv // 2
    rows, D = hidden.shape
    V = embedding.shape[0]
    K = D // ck
    part = rows // NH
    TH = nd * part
    d, v = lax.axis_index("dp"), lax.axis_index("vocab")
    c, y = lax.rem(d, 2), d // 2
    x, z = lax.rem(v, 2), v // 2
    dev = lambda dd, vv: dict(device_id=(dd, vv), device_id_type=MESH)
    core = dev(y * 2 + 1 - c, v)
    xdev = dev(d, z * 2 + 1 - x)
    ydev = lambda k: dev(lax.rem(y + k, Y) * 2 + c, v)
    zdev = lambda k: dev(d, lax.rem(z + k, Z) * 2 + x)
    ddev = lambda k: dev(lax.rem(d + k, nd), v)
    vdev = lambda k: dev(d, lax.rem(v + k, nv))
    rdma = lambda s, t, ss, rs, dv: pltpu.make_async_remote_copy(src_ref=s, dst_ref=t, send_sem=ss, recv_sem=rs, **dv)

    block = lambda dd, a: hid.at[pl.ds(pl.multiple_of(a * TH + dd * part, part), part)]
    loads = [pltpu.make_async_copy(hidden.at[pl.ds(a * part, part)], block(d, a), loc.at[a]) for a in range(NH)]
    load_e = pltpu.make_async_copy(embedding, emb, loc.at[NH])
    for copy in loads:
        copy.start()
    load_e.start()
    barrier = pltpu.get_barrier_semaphore()
    for k in range(1, nd):
        pl.semaphore_signal(barrier, inc=1, **ddev(k))
    for k in range(1, nv):
        pl.semaphore_signal(barrier, inc=1, **vdev(k))
    T = NH * TH
    at = lax.broadcasted_iota(jnp.int32, (rows, T), 1)
    own = lax.broadcasted_iota(jnp.int32, (rows, T), 0)
    place = jnp.where((own // part) * TH + d * part + lax.rem(own, part) == at, 1.0, 0.0)
    line = jnp.concatenate([weights[...], targets[...].astype(f32), jnp.zeros((6, rows), f32)], axis=0)
    tw[0] = jnp.dot(line, place, precision=lax.Precision.HIGHEST, preferred_element_type=f32)
    for copy in loads:
        copy.wait()
    pl.semaphore_wait(barrier, nd + nv - 2)

    sends = []

    def go(copy):
        copy.start()
        sends.append(copy)
        return copy

    hy = lambda a, k: rdma(block(d, a), block(d, a), hy_s.at[a, k - 1], hy_r.at[a, k - 1], ydev(k))
    hc = lambda a: rdma(block(d, a), block(d, a), hc_s.at[a], hc_r.at[a], core)

    def hf(a, k):
        there = block(lax.rem(y + Y - k, Y) * 2 + c, a)
        return rdma(there, there, hf_s.at[a, k - 1], hf_r.at[a, k - 1], core)

    twc = lambda k: rdma(tw.at[0], tw.at[k], tw_s.at[k - 1], tw_r.at[k - 1], ddev(k))
    for k in range(1, nd):
        go(twc(k))
    for a in range(NH):
        for k in range(1, Y):
            go(hy(a, k))
        go(hc(a))

    def forward(a):
        for k in range(1, Y):
            hy(a, k).wait_recv()
            go(hf(a, k))

    def arrived(a):
        hc(a).wait_recv()
        for k in range(1, Y):
            hf(a, k).wait_recv()

    def logits(a):
        pd[a, 0] = jnp.zeros_like(pd[a, 0])

        def step(b, carry):
            vb = pl.ds(pl.multiple_of(b * VB, VB), VB)
            lg = lax.dot_general(emb[vb, :], hid[a * TH:(a + 1) * TH, :], (((1,), (1,)), ((), ())), preferred_element_type=f32)
            u = jnp.tanh(lg * (1.0 / soft_cap))
            e = jnp.exp(soft_cap * u - soft_cap)
            uT[a, vb, :] = 1.0 - u * u
            eT[a, vb, :] = e
            pd[a, 0] += jnp.sum(e.reshape(VB // 8, 8, TH), axis=0)
            return carry

        lax.fori_loop(0, V // VB, step, 0)

    pdc = lambda a, k: rdma(pd.at[a, 0], pd.at[a, k], pd_s.at[a, k - 1], pd_r.at[a, k - 1], ddev(k))
    pvc = lambda a, k: rdma(pv.at[a, 0], pv.at[a, k], pv_s.at[a, k - 1], pv_r.at[a, k - 1], vdev(k))

    def sums_out(a):
        for k in range(1, nd):
            go(pdc(a, k))

    def sums_on(a):
        for k in range(1, nd):
            pdc(a, k).wait_recv()
        pv[a, 0] = jnp.sum(pd[a], axis=0)
        for k in range(1, nv):
            go(pvc(a, k))

    first = (d * nv + v) * V

    def scores(a):
        for k in range(1, nv):
            pvc(a, k).wait_recv()
        total = jnp.sum(jnp.sum(pv[a], axis=0), axis=0, keepdims=True)
        group = jnp.sum(tw[:, :, a * TH:(a + 1) * TH], axis=0)
        weight, target = group[0:1, :], group[1:2, :]
        factor = weight * (1.0 + 2.0 * z_weight * (soft_cap + jnp.log(total))) / total

        def step(b, carry):
            vb = pl.ds(pl.multiple_of(b * VB, VB), VB)
            cols = (first + b * VB + lax.broadcasted_iota(jnp.int32, (VB, TH), 0)).astype(f32)
            s = (factor * eT[a, vb, :] - jnp.where(cols == target, weight, 0.0)) * uT[a, vb, :]
            sT[vb, a * TH:(a + 1) * TH] = s.astype(bf16)
            sN[a * TH:(a + 1) * TH, vb] = s.T.astype(bf16)
            return carry

        lax.fori_loop(0, V // VB, step, 0)

    ccopy = lambda i: rdma(sC.at[i], rC.at[i], c_s.at[i], c_r.at[i], core)
    ycopy = lambda i, k: rdma(sY.at[i, k - 1], rY.at[i, k - 1], y_s.at[i, k - 1], y_r.at[i, k - 1], ydev(k))

    def core_unit(i):
        ccopy(i).wait()
        for k in range(1, Y):
            yy = lax.rem(y + k, Y)
            sY[i, k - 1] = (gF[i, yy * 2 + c] + rC[i, yy].astype(f32)).astype(bf16)
            ycopy(i, k).start()

    def partials(a):
        def step(j, carry):
            i = a * K + j
            g = jnp.dot(sN[a * TH:(a + 1) * TH, :], emb[:, pl.ds(pl.multiple_of(j * ck, ck), ck)], preferred_element_type=f32)
            gF[i] = g.reshape(nd, part, ck)
            for yy in range(Y):
                sC[i, yy] = gF[i, yy * 2 + 1 - c].astype(bf16)
            ccopy(i).start()

            @pl.when(j >= 2)
            def _():
                core_unit(i - 2)

            return carry

        lax.fori_loop(0, K, step, 0)
        for j in range(max(K - 2, 0), K):
            core_unit(a * K + j)

    forward(0)
    for k in range(1, nd):
        twc(k).wait_recv()
    arrived(0)
    load_e.wait()
    logits(0)
    sums_out(0)
    for a in range(1, NH):
        forward(a)
        sums_on(a - 1)
        arrived(a)
        logits(a)
        sums_out(a)
        scores(a - 1)
        sums_on(a)
        partials(a - 1)
    if NH == 1:
        sums_on(0)
    scores(NH - 1)
    partials(NH - 1)

    pieces = [(b, j) for b in range(V // VB) for j in range(D // TC)]

    def table(b, j):
        vb, cs = pl.ds(b * VB, VB), pl.ds(j * TC, TC)
        tgrad[vb, cs] = jnp.dot(sT[vb, :], hid[:, cs], preferred_element_type=f32).astype(bf16)

    U = NH * K

    def y_unit(i):
        acc = gF[i, y * 2 + c] + rC[i, y].astype(f32)
        for k in range(1, Y):
            ycopy(i, k).wait()
            acc = acc + rY[i, k - 1].astype(f32)
        return acc

    if not full:
        for piece in pieces:
            table(*piece)
        for i in range(U):
            a, j = i // K, i % K
            hgrad[a * part:(a + 1) * part, j * ck:(j + 1) * ck] = y_unit(i)
    else:
        h = part // 8
        gz = h // Z
        cx = ck // 2
        xcopy = lambda i: rdma(sX.at[i], rX.at[i], x_s.at[i], x_r.at[i], xdev)
        zcopy = lambda i, k: rdma(sZ.at[i, k - 1], rZ.at[i, k - 1], z_s.at[i, k - 1], z_r.at[i, k - 1], zdev(k))
        mycols = lambda i: pl.ds(pl.multiple_of((i % K) * ck + x * cx, cx), cx)
        mine = lambda i: out.at[pl.ds((i // K) * h + z * gz, gz), :, mycols(i)]
        half = lambda i: out.at[pl.ds((i // K) * h, h), :, mycols(i)]
        azcopy = lambda i, k: rdma(mine(i), mine(i), az_s.at[i, k - 1], az_r.at[i, k - 1], zdev(k))
        axcopy = lambda i: rdma(half(i), half(i), ax_s.at[i], ax_r.at[i], xdev)
        xsum = lambda i, zz: bF[i, x, pl.ds(zz * gz, gz)] + rX[i, pl.ds(zz * gz, gz)].astype(f32)

        def stage0(i):
            acc = y_unit(i).reshape(h, 8, ck)
            for xx in range(2):
                bF[i, xx] = acc[:, :, xx * cx:(xx + 1) * cx]
            sX[i] = bF[i, 1 - x].astype(bf16)
            xcopy(i).start()

        def stage1(i):
            xcopy(i).wait()
            for k in range(1, Z):
                sZ[i, k - 1] = xsum(i, lax.rem(z + k, Z)).astype(bf16)
                zcopy(i, k).start()

        def stage2(i):
            acc = xsum(i, z)
            for k in range(1, Z):
                zcopy(i, k).wait()
                acc = acc + rZ[i, k - 1].astype(f32)
            out[pl.ds((i // K) * h + z * gz, gz), :, mycols(i)] = acc.astype(bf16)
            for k in range(1, Z):
                azcopy(i, k).start()

        def stage3(i):
            for k in range(1, Z):
                azcopy(i, k).wait()
            axcopy(i).start()

        def filler(count):
            for _ in range(count):
                if pieces:
                    table(*pieces.pop(0))

        def run(stage, a):
            for i in range(a * K, (a + 1) * K):
                stage(i)

        third = -(-len(pieces) // 3)
        run(stage0, 0)
        filler(third)
        for a in range(NH):
            run(stage1, a)
            filler(third)
            if a + 1 < NH:
                run(stage0, a + 1)
                filler(third)
            if a > 0:
                run(stage3, a - 1)
            run(stage2, a)
        run(stage3, NH - 1)
        for piece in pieces:
            table(*piece)
        for i in range(U):
            axcopy(i).wait()
        hgrad[...] = out[...]
    for copy in sends:
        copy.wait_send()


def body(hidden, embedding, targets, loss_weight):
    nd, nv = lax.axis_size("dp"), lax.axis_size("vocab")
    rows, D = hidden.shape
    V = embedding.shape[0]
    T = rows * nd
    Y, Z = nd // 2, nv // 2
    ck = next(s for s in (1792, 512, 256, D) if D % s == 0)
    TC = next(s for s in (896, 512, 256, 128, D) if D % s == 0)
    K = D // ck
    NH = 2
    VB = next(s for s in (256, 128, V) if V % s == 0)
    part = rows // NH
    TH = nd * part
    U = NH * K
    full = (part // 8) % Z == 0
    h = part // 8
    gz = max(h // Z, 1)
    cx = ck // 2
    Zs, Ys = max(Z - 1, 1), max(Y - 1, 1)
    VM = pltpu.VMEM
    dma = lambda *shape: pltpu.SemaphoreType.DMA(shape)
    scratch = [
        VM((T, D), bf16), VM((V, D), bf16), VM((nd, 8, T), f32), VM((NH, nd, 8, TH), f32), VM((NH, nv, 8, TH), f32),
        VM((NH, V, TH), f32), VM((NH, V, TH), f32), VM((V, T), bf16), VM((T, V), bf16),
        VM((U, nd, part, ck), f32), VM((U, Y, part, ck), bf16), VM((U, Y, part, ck), bf16),
        VM((U, Ys, part, ck), bf16), VM((U, Ys, part, ck), bf16),
        VM((U, 2, h, 8, cx), f32), VM((U, h, 8, cx), bf16), VM((U, h, 8, cx), bf16),
        VM((U, Zs, gz, 8, cx), bf16), VM((U, Zs, gz, 8, cx), bf16),
        VM((NH * h, 8, D), bf16),
        dma(NH + 1), dma(nd), dma(nd), dma(NH), dma(NH), dma(NH, Ys), dma(NH, Ys), dma(NH, Ys), dma(NH, Ys),
        dma(NH, nd), dma(NH, nd), dma(NH, nv), dma(NH, nv),
        dma(U), dma(U), dma(U, Ys), dma(U, Ys), dma(U), dma(U), dma(U, Zs), dma(U, Zs), dma(U, Zs), dma(U, Zs), dma(U), dma(U),
    ]
    hshape = jax.ShapeDtypeStruct((NH * h, 8, D), bf16) if full else jax.ShapeDtypeStruct((rows, D), f32)
    any_spec = pl.BlockSpec(memory_space=pltpu.HBM)
    vmem_spec = pl.BlockSpec(memory_space=pltpu.VMEM)
    hgrad, tgrad = pl.pallas_call(
        functools.partial(kernel, (nd, nv, full, ck, NH, VB, TC)),
        out_shape=(hshape, jax.ShapeDtypeStruct((V, D), bf16)),
        in_specs=[any_spec, any_spec, vmem_spec, vmem_spec],
        out_specs=(vmem_spec, vmem_spec),
        scratch_shapes=scratch,
        compiler_params=pltpu.CompilerParams(collective_id=0, has_side_effects=True, vmem_limit_bytes=VMEM_LIMIT * 1024 * 1024),
    )(hidden, embedding, targets.reshape(1, rows), loss_weight.astype(f32).reshape(1, rows))
    if full:
        return hgrad.reshape(rows, D), tgrad
    return lax.psum(hgrad, "vocab").astype(bf16), tgrad


def solution(mesh):
    return jax.shard_map(
        body,
        mesh=mesh,
        in_specs=(P("dp", None), P(("dp", "vocab"), None), P("dp"), P("dp")),
        out_specs=(P("dp", None), P(("dp", "vocab"), None)),
        check_vma=False,
    )
```
